32 devices in a mesh: gx: 4 (over z), gy: 4 (over x, core), gz: 2 (over y).
Axes of the slice: x: 2, y: 2, z: 4, core: 2. Of those that a mesh axis runs over, the one named last changes fastest.
Arguments:
- blocks: bfloat16 [4, 4, 128, 256, 256], P('gy', 'gx'), may hold values from -0.0625 to 0.0625
- block_rows: int32 [4, 4, 128], P('gy', 'gx'), may hold values from 0 to 15
- block_cols: int32 [4, 4, 128], P('gy', 'gx'), may hold values from 0 to 15
- probe_bits: int32 [16384, 256], P(('gy', 'gx'), 'gz'), may hold values from 0 to 1
- shift: float32 [16384], P(('gy', 'gx')), may hold values from 0 to 0.7
Outputs:
- forms: float32 [3, 256], P(None, 'gz')
- last_term: float32 [16384, 256], P(('gy', 'gx'), 'gz')
The draws below stay inside these ranges and needn't reach their ends.
All inputs are finite; a program needn't handle non-finite values.
Results may differ from the reference program's by a relative error of at most 0.02.
Values may be sent and summed in bfloat16 or wider, within the bound.
No kernel may reach another device: no remote copies, remote signals or barrier semaphores. Data moves between devices by JAX's collectives and lax.ppermute only.
A program may use at most 128 MiB of HBM per device.

```python
import jax
import jax.numpy as jnp
from jax import lax

BS = 256
RB_DEV = 4
KT = 128
NB = 64
NV = 16384
PROBES = 256
TROWS = 16
TCOLS = 16
N_GX = 4
N_GY = 4


def draw_shift(key, part):
    positions = jnp.arange(NV, dtype=jnp.int32)
    group = TROWS * BS
    across = (positions % group).astype(jnp.float32) / group
    upward = (positions // group).astype(jnp.float32) / (NV // group)
    rough = jax.random.uniform(key, (NV,), jnp.float32, -0.1, 0.1)
    return (0.1 + 0.4 * across + 0.1 * upward + rough).astype(jnp.float32)


def touch_ends(values, key, smallest, top_value):
    spot = [jax.random.randint(jax.random.fold_in(key, axis), (), 0, length) for axis, length in enumerate(values.shape)]
    main_axis = values.shape.index(max(values.shape))
    beside = spot[:main_axis] + [(spot[main_axis] + 1) % values.shape[main_axis]] + spot[main_axis + 1:]
    return values.at[tuple(spot)].set(smallest).at[tuple(beside)].set(top_value)


def block_scale(stream_key, shape, split, least, high):
    def one(axis_at, blocks):
        heights = jax.random.uniform(jax.random.fold_in(jax.random.fold_in(stream_key, 6), axis_at), (blocks,), jnp.float32, least / len(split), high / len(split))
        return jnp.repeat(jnp.exp(heights), shape[axis_at] // blocks).reshape((-1,) + (1,) * (len(shape) - axis_at - 1))

    level = one(*split[0])
    for cut in split[1:]:
        level = level * one(*cut)
    return level


def bell_draw(key, dims, scale, most, cuts=(), kind=jnp.bfloat16):
    loudness = block_scale(key, dims, cuts, -0.22, 0.18) if cuts else 1.0
    entries = jax.random.normal(key, dims, jnp.float32) * scale * loudness
    return jnp.minimum(jnp.maximum(entries, -most), most).astype(kind)


def setup_inputs(seed: int = 0) -> dict:
    streams_of = jax.random.split(jax.random.key(seed), 6)
    return {
        "blocks": bell_draw(streams_of[0], (N_GY, N_GX, KT, BS, BS), (KT * BS // RB_DEV) ** -0.5, 0.0625, ((0, 4), (1, 4))),
        "block_rows": touch_ends(jax.random.randint(streams_of[1], (N_GY, N_GX, KT), 0, TROWS), jax.random.fold_in(streams_of[1], 1), 0, TROWS - 1).astype(jnp.int32),
        "block_cols": touch_ends(jax.random.randint(streams_of[2], (N_GY, N_GX, KT), 0, TCOLS), jax.random.fold_in(streams_of[2], 1), 0, TCOLS - 1).astype(jnp.int32),
        "probe_bits": touch_ends(jax.random.randint(streams_of[3], (NV, PROBES), 0, 2), jax.random.fold_in(streams_of[3], 1), 0, 1).astype(jnp.int32),
        "shift": draw_shift(jax.random.fold_in(streams_of[5], 71), 0),
    }


def apply_operator(blocks, block_rows, block_cols, shift, field):
    rounded = field.astype(jnp.bfloat16).reshape(NB, BS, PROBES)
    flat_blocks = blocks.reshape(N_GY * N_GX, KT, BS, BS)
    flat_rows = block_rows.reshape(N_GY * N_GX, KT)
    flat_cols = block_cols.reshape(N_GY * N_GX, KT)
    tile_ids = jnp.arange(N_GY * N_GX, dtype=jnp.int32)

    def one_tile(total, items):
        tile_blocks, rows_here, cols_here, tile = items
        row_group = (tile // N_GX).astype(jnp.int32)
        col_group = tile % N_GX
        global_cols = ((cols_here // RB_DEV) * TROWS + col_group * RB_DEV + cols_here % RB_DEV).astype(jnp.int32)
        picked = rounded[global_cols].astype(jnp.float32)
        product = jnp.einsum('kab,kbp->kap', tile_blocks.astype(jnp.float32), picked)
        partial_value = jnp.zeros((TROWS, BS, PROBES), jnp.float32).at[rows_here.astype(jnp.int32)].add(product)
        partial_value = lax.optimization_barrier(partial_value.astype(jnp.bfloat16)).astype(jnp.float32)
        return total.at[row_group].add(partial_value), None

    start = jnp.zeros((N_GY, TROWS, BS, PROBES), jnp.float32)
    total, _ = lax.scan(one_tile, start, (flat_blocks, flat_rows, flat_cols, tile_ids))
    return total.reshape(NV, PROBES) + shift[:, None] * field


def reference(blocks, block_rows, block_cols, probe_bits, shift):
    signs = (2 * probe_bits - 1).astype(jnp.float32)
    first = apply_operator(blocks, block_rows, block_cols, shift, signs)
    second = 2.0 * apply_operator(blocks, block_rows, block_cols, shift, first) - signs
    third = 2.0 * apply_operator(blocks, block_rows, block_cols, shift, second) - first
    forms = jnp.stack([jnp.sum(signs * first, axis=0), jnp.sum(signs * second, axis=0), jnp.sum(signs * third, axis=0)])
    return forms, third
```

```python
import functools

import jax
import jax.numpy as jnp
from jax import lax
from jax.experimental import pallas as pl
from jax.experimental.pallas import tpu as pltpu
from jax.sharding import PartitionSpec as P

UNROLL = 8
VMEM = pl.BlockSpec(memory_space=pltpu.VMEM)
SMEM = pl.BlockSpec(memory_space=pltpu.SMEM)


def swap(value, axis, mask):
    n = lax.axis_size(axis)
    return lax.ppermute(value, axis, [(d, d ^ mask) for d in range(n)])


def multiply_kernel(pieces, slots, groups, plan_ref, blocks_ref, *refs):
    piece_refs = refs[:pieces]
    send_ref, keep_ref, field, total = refs[pieces:]
    size = blocks_ref.shape[1]
    rows = piece_refs[0].shape[0]
    for m, piece in enumerate(piece_refs):
        field[pl.ds(m * rows, rows), :] = piece[...]
    field[pl.ds(pieces * rows, size), :] = jnp.zeros((size, field.shape[1]), field.dtype)
    total[...] = jnp.zeros_like(total)

    def step(it, carry):
        for u in range(UNROLL):
            at = it * UNROLL + u
            col = plan_ref[1, at]
            row = plan_ref[2, at]
            part = jnp.dot(
                blocks_ref[plan_ref[0, at]],
                field[pl.ds(pl.multiple_of(col * size, size), size), :],
                preferred_element_type=jnp.float32,
            )
            total[row] += part
        return carry

    lax.fori_loop(0, plan_ref[3, 0], step, 0)
    half = total.shape[0] // 2
    keep_ref[...] = total[:half].reshape(keep_ref.shape)
    send_ref[...] = total[half:].reshape(send_ref.shape).astype(send_ref.dtype)


def make_plan(block_rows, block_cols, rb, n_gx, n_gy):
    kt = block_rows.shape[0]
    slots = kt + UNROLL
    here_x, here_y = lax.axis_index("gx"), lax.axis_index("gy")
    dest = (block_rows // rb) ^ here_x
    row = ((dest & 1) * (n_gx // 2) + dest // 2) * rb + block_rows % rb
    col = ((block_cols // rb) ^ here_y) * rb + block_cols % rb
    ids = jnp.arange(kt, dtype=jnp.int32)
    before = (row[None, :] > row[:, None]) | (
        (row[None, :] == row[:, None]) & (ids[None, :] < ids[:, None])
    )
    place = jnp.sum(before.astype(jnp.int32), axis=1)
    hit = place[None, :] == jnp.arange(slots, dtype=jnp.int32)[:, None]
    pick = lambda v, fill: jnp.sum(jnp.where(hit, v[None, :] - fill, 0), axis=1) + fill
    count = jnp.full((slots,), (kt + UNROLL - 1) // UNROLL, jnp.int32)
    return jnp.stack([pick(ids, 0), pick(col, n_gy * rb), pick(row, 0), count])


def body(blocks, block_rows, block_cols, probe_bits, shift):
    tile_blocks = blocks[0, 0]
    kt, size, _ = tile_blocks.shape
    local_rows, probes = probe_bits.shape
    rb = local_rows // size
    n_gx, n_gy = lax.axis_size("gx"), lax.axis_size("gy")
    plan = make_plan(block_rows[0, 0], block_cols[0, 0], rb, n_gx, n_gy)
    signs = (2 * probe_bits - 1).astype(jnp.float32)

    def apply_operator(field):
        pieces = [field.astype(jnp.bfloat16)]
        mask = n_gy // 2
        own = {0: pieces[0]}
        while mask:
            own.update({m | mask: swap(v, "gy", mask) for m, v in own.items()})
            mask //= 2
        pieces = [own[m] for m in range(n_gy)]
        half = n_gx // 2 * local_rows
        send, keep = pl.pallas_call(
            functools.partial(multiply_kernel, n_gy, plan.shape[1], 1),
            out_shape=(
                jax.ShapeDtypeStruct((half, probes), jnp.bfloat16),
                jax.ShapeDtypeStruct((half, probes), jnp.float32),
            ),
            in_specs=[SMEM, VMEM] + [VMEM] * n_gy,
            out_specs=(VMEM, VMEM),
            scratch_shapes=[
                pltpu.VMEM(((n_gy * rb + 1) * size, probes), jnp.bfloat16),
                pltpu.VMEM((n_gx * rb, size, probes), jnp.float32),
            ],
            compiler_params=pltpu.CompilerParams(vmem_limit_bytes=60 << 20),
            cost_estimate=pl.CostEstimate(
                flops=2 * kt * size * size * probes, bytes_accessed=kt * size * size * 2, transcendentals=0
            ),
            name="multiply",
        )(plan, tile_blocks, *pieces)
        mask, width = 1, n_gx // 2
        while True:
            keep = keep + swap(send, "gx", mask).astype(jnp.float32)
            mask *= 2
            if mask == n_gx:
                break
            parts = keep.reshape(width // 2, 2, local_rows, probes)
            send = parts[:, 1].reshape(-1, probes).astype(jnp.bfloat16)
            keep = parts[:, 0].reshape(-1, probes)
            width //= 2
        return keep + shift[:, None] * field

    first = apply_operator(signs)
    second = 2.0 * apply_operator(first) - signs
    third = 2.0 * apply_operator(second) - first
    forms = jnp.stack([jnp.sum(signs * term, axis=0) for term in (first, second, third)])
    for axis in ("gy", "gx"):
        mask = 1
        while mask < lax.axis_size(axis):
            forms = forms + swap(forms, axis, mask)
            mask *= 2
    return (forms, third)


def solution(mesh):
    return jax.shard_map(
        body,
        mesh=mesh,
        in_specs=(
            P("gy", "gx", None, None, None),
            P("gy", "gx", None),
            P("gy", "gx", None),
            P(("gy", "gx"), "gz"),
            P(("gy", "gx")),
        ),
        out_specs=(P(None, "gz"), P(("gy", "gx"), "gz")),
        check_vma=False,
    )
```

```python
import functools

import jax
import jax.numpy as jnp
from jax import lax
from jax.experimental import pallas as pl
from jax.experimental.pallas import tpu as pltpu
from jax.sharding import PartitionSpec as P


WIDE, NARROW = 16, 8
VMEM = pl.BlockSpec(memory_space=pltpu.VMEM)
ANY = pl.BlockSpec(memory_space=pl.ANY)
PARAMS = pltpu.CompilerParams(vmem_limit_bytes=24 << 20)


def swap(value, axis, mask):
    n = lax.axis_size(axis)
    return lax.ppermute(value, axis, [(d, d ^ mask) for d in range(n)])


def after(value, gate):
    return lax.optimization_barrier((value, gate))[0]


class Layout:
    def __init__(self, kt, size, probes, rb, n_gx, n_gy):
        self.kt, self.size, self.probes, self.rb, self.n_gx, self.n_gy = kt, size, probes, rb, n_gx, n_gy
        self.top, self.dests = n_gy // 2, n_gx // 2
        small = max(rb // 4, 1)
        self.chunks = [rb - rb // 2, rb // 2]
        self.starts = [sum(self.chunks[:c]) for c in range(len(self.chunks))]
        self.steps = (WIDE, WIDE, NARROW, NARROW)
        tail = self.chunks[-1]
        self.last = rb - tail
        self.fields = (self.top * self.last, self.top * rb, self.top * tail, self.top * tail)
        self.firsts = (0, 0, self.dests * rb, 0)
        self.slots = -(-(kt + sum(self.steps)) // 128) * 128

    def place(self, block_rows, block_cols):
        rb, here_x, here_y = self.rb, lax.axis_index("gx"), lax.axis_index("gy")
        dest, q = (block_rows // rb) ^ here_x, block_rows % rb
        piece, blk = (block_cols // rb) ^ here_y, block_cols % rb
        send = dest % 2
        row = send * (self.dests * rb)
        col = jnp.zeros_like(blk)
        for start, count in zip(self.starts, self.chunks):
            inside = (q >= start) & (q < start + count)
            row += jnp.where(inside, self.dests * start + dest // 2 * count + q - start, 0)
            inside = (blk >= start) & (blk < start + count)
            col += jnp.where(inside, self.top * start + piece % self.top * count + blk - start, 0)
        near, soon = piece < self.top, blk < self.last
        col -= jnp.where(near | soon, 0, self.top * self.last)
        which = jnp.where(near & soon, 0, jnp.where(near | soon, 1, 3 - send))
        return which, col, row


def start_kernel(lay, rows_hbm, cols_hbm, blocks_ref, held_ref, plan_ref, rows_ref, cols_ref, sem):
    kt, parts = lay.kt, sem.shape[0] - 2
    small = [
        pltpu.make_async_copy(rows_hbm, rows_ref, sem.at[parts]),
        pltpu.make_async_copy(cols_hbm, cols_ref, sem.at[parts + 1]),
    ]
    for copy in small:
        copy.start()
    cut = lambda ref, p: ref.at[pl.ds(p * (kt // parts), kt // parts)]
    copies = [pltpu.make_async_copy(cut(blocks_ref, p), cut(held_ref, p), sem.at[p]) for p in range(parts)]
    for copy in copies:
        copy.start()
    for copy in small:
        copy.wait()
    down, along = (lax.broadcasted_iota(jnp.int32, (kt, kt), d) for d in (0, 1))
    upright = lambda v: jnp.sum(jnp.where(down == along, v, 0), axis=1, keepdims=True)
    flat = lay.place(rows_ref[...], cols_ref[...])
    which, col, row = (upright(v) for v in flat)
    rank = jnp.sum(((flat[0] == which) & (along < down)).astype(jnp.int32), axis=1, keepdims=True)
    slots = lax.broadcasted_iota(jnp.int32, (1, lay.slots), 1)
    place, base = rank, jnp.zeros((1, 1), jnp.int32)
    fill_col, fill_row = jnp.zeros_like(slots), jnp.zeros_like(slots)
    sizes = jnp.zeros_like(slots)
    for number, step in enumerate(lay.steps):
        count = jnp.sum((flat[0] == number).astype(jnp.int32), axis=1, keepdims=True)
        trips = (count + step - 1) // step
        place += jnp.where(which == number, base, 0)
        end = base + trips * step
        inside = (slots >= base) & (slots < end)
        fill_col += jnp.where(inside, lay.fields[number], 0)
        fill_row += jnp.where(inside, lay.firsts[number], 0)
        sizes += jnp.where(slots == 2 * number, base, 0) + jnp.where(slots == 2 * number + 1, trips, 0)
        base = end
    hit = place == slots
    pick = lambda v: jnp.sum(jnp.where(hit, v, 0), axis=0, keepdims=True)
    empty = 1 - pick(1)
    plan_ref[0:1, :] = pick(lax.broadcasted_iota(jnp.int32, (kt, 1), 0))
    plan_ref[1:2, :] = pick(col) + empty * fill_col
    plan_ref[2:3, :] = pick(row) + empty * fill_row
    plan_ref[3:4, :] = sizes
    for copy in copies:
        copy.wait()


def run_list(lay, number, plan_hbm, blocks_ref, pieces, field, total, plan_ref, sem, prepare):
    size, first_row, step = lay.size, lay.firsts[number], lay.steps[number]
    fetch = pltpu.make_async_copy(plan_hbm, plan_ref, sem)
    fetch.start()
    prepare()
    place = 0
    for piece in pieces:
        field[pl.ds(place, piece.shape[0]), :] = piece[...]
        place += piece.shape[0]
    field[pl.ds(place, size), :] = jnp.zeros((size, lay.probes), field.dtype)
    fetch.wait()
    start = plan_ref[3, 2 * number]

    def go(it, carry):
        for u in range(step):
            at = start + it * step + u
            part = jnp.dot(
                blocks_ref[plan_ref[0, at]],
                field[pl.ds(pl.multiple_of(plan_ref[1, at] * size, size), size), :],
                preferred_element_type=jnp.float32,
            )
            total[plan_ref[2, at] - first_row] += part
        return carry

    lax.fori_loop(0, plan_ref[3, 2 * number + 1], go, 0)


def early_kernel(lay, number, plan_hbm, blocks_ref, *refs):
    before, refs = (refs[0], refs[1:]) if number else (None, refs)
    *pieces, total, field, plan_ref, sem = refs

    def prepare():
        total[...] = jnp.zeros_like(total) if before is None else before[...]

    run_list(lay, number, plan_hbm, blocks_ref, pieces, field, total, plan_ref, sem, prepare)


def late_kernel(lay, number, plan_hbm, blocks_ref, before, *refs):
    pieces, outs = refs[: lay.top], refs[lay.top : -4]
    field, total, plan_ref, sem = refs[-4:]

    def prepare():
        total[...] = before[pl.ds(lay.firsts[number], total.shape[0])]

    run_list(lay, number, plan_hbm, blocks_ref, pieces, field, total, plan_ref, sem, prepare)
    for out, start, count in zip(outs, lay.starts, lay.chunks):
        part = total[pl.ds(lay.dests * start, lay.dests * count)]
        out[...] = part.reshape(out.shape).astype(out.dtype)


def body(blocks, block_rows, block_cols, probe_bits, shift):
    kt, size, _ = blocks.shape[2:]
    local_rows, probes = probe_bits.shape
    n_gx, n_gy = lax.axis_size("gx"), lax.axis_size("gy")
    lay = Layout(kt, size, probes, local_rows // size, n_gx, n_gy)
    chunks = range(len(lay.chunks))

    def cost(share):
        return pl.CostEstimate(
            flops=int(2 * kt * size * size * probes * share), bytes_accessed=0, transcendentals=0
        )

    cut = lambda v: [v[s * size : (s + n) * size] for s, n in zip(lay.starts, lay.chunks)]
    signs = [(2 * v - 1).astype(jnp.float32) for v in cut(probe_bits)]
    scale = [v[:, None] for v in cut(shift)]

    begin = pl.pallas_call(
        functools.partial(start_kernel, lay),
        out_shape=(
            jax.ShapeDtypeStruct((kt, size, size), blocks.dtype),
            jax.ShapeDtypeStruct((4, lay.slots), jnp.int32),
        ),
        in_specs=[ANY, ANY, ANY],
        out_specs=(VMEM, VMEM),
        scratch_shapes=[
            pltpu.VMEM((1, kt), jnp.int32),
            pltpu.VMEM((1, kt), jnp.int32),
            pltpu.SemaphoreType.DMA((10,)),
        ],
        compiler_params=PARAMS,
        cost_estimate=cost(1.0),
        name="start",
    )
    held, plan = begin(block_rows[0], block_cols[0], blocks[0, 0])

    def spread(pieces):
        own, mask = {0: pieces}, lay.top // 2
        while mask:
            own.update({m | mask: swap(v, "gy", mask) for m, v in own.items()})
            mask //= 2
        return [own[m] for m in range(lay.top)]

    fetched = [pltpu.SMEM((4, lay.slots), jnp.int32), pltpu.SemaphoreType.DMA]

    def early(number, before, pieces, share):
        return pl.pallas_call(
            functools.partial(early_kernel, lay, number),
            out_shape=jax.ShapeDtypeStruct((n_gx * lay.rb, size, probes), jnp.float32),
            in_specs=[ANY, VMEM] + [VMEM] * (len(before) + len(pieces)),
            out_specs=VMEM,
            scratch_shapes=[pltpu.VMEM(((lay.fields[number] + 1) * size, probes), jnp.bfloat16)] + fetched,
            compiler_params=PARAMS,
            cost_estimate=cost(share),
        )(plan, held, *before, *pieces)

    def late(number, dtype, before, pieces, share):
        return pl.pallas_call(
            functools.partial(late_kernel, lay, number),
            out_shape=tuple(jax.ShapeDtypeStruct((lay.dests * n * size, probes), dtype) for n in lay.chunks),
            in_specs=[ANY, VMEM, VMEM] + [VMEM] * len(pieces),
            out_specs=(VMEM,) * len(lay.chunks),
            scratch_shapes=[
                pltpu.VMEM(((lay.fields[number] + 1) * size, probes), jnp.bfloat16),
                pltpu.VMEM((lay.dests * lay.rb, size, probes), jnp.float32),
            ]
            + fetched,
            compiler_params=PARAMS,
            cost_estimate=cost(share),
        )(plan, held, before, *pieces)

    def multiply(field):
        across = [swap(v, "gy", lay.top) for v in field]
        near = [spread(v) for v in field]
        far = [spread(v) for v in across[:-1]]
        total = early(0, [], sum(near[:-1], []), 0.25)
        total = early(1, [total], sum(far, []) + near[-1], 0.5)
        rest = spread(after(across[-1], total))
        send = late(2, jnp.bfloat16, total, rest, 0.12)
        return send, late(3, jnp.float32, total, rest, 0.12)

    def reduce(send, keep, gate=None):
        send, keep, last = list(send), list(keep), [None] * len(send)
        mask, width = 1, n_gx // 2
        while True:
            got = [swap(v, "gx", mask) for v in send]
            mask *= 2
            if mask == n_gx and gate is not None:
                sums = gate(last)
                got[0] = after(got[0], sums[0])
                got[-1] = after(got[-1], sums[1])
            for c in chunks:
                if c:
                    got[c] = after(got[c], send[c - 1] if mask < n_gx else keep[c - 1])
                keep[c] = keep[c] + got[c].astype(jnp.float32)
                if mask < n_gx:
                    parts = keep[c].reshape(width // 2, 2, -1, probes)
                    keep[c] = parts[:, 0].reshape(-1, probes)
                    gone = parts[:, 1].reshape(-1, probes)
                    last[c] = (keep[c], gone)
                    send[c] = gone.astype(jnp.bfloat16)
            width //= 2
            if mask == n_gx:
                return keep

    def apply_operator(field, previous, factor, gate=None):
        send, keep = multiply([v.astype(jnp.bfloat16) for v in field])
        sums = reduce(send, keep, gate)
        out = []
        for s, d, v, u in zip(sums, scale, field, previous):
            if out:
                s = after(s, out[-1].astype(jnp.bfloat16))
            term = factor * (s + d * v)
            out.append(term if u is None else term - u)
        return out

    def dot(us, vs):
        return sum(jnp.sum(u * v, axis=0) for u, v in zip(us, vs))

    far_signs = [swap(v.astype(jnp.bfloat16), "gx", n_gx // 2).astype(jnp.float32) for v in signs]
    first = apply_operator(signs, [None] * len(signs), 1.0)
    second = apply_operator(first, signs, 2.0)
    forms = []

    def add_forms(last):
        rest = [2.0 * d * v - u for d, v, u in zip(scale, second, first)]
        form3 = dot(signs, rest)
        form3 += 2.0 * (dot(signs, [v[0] for v in last]) + dot(far_signs, [v[1] for v in last]))
        total = jnp.stack([dot(signs, first), dot(signs, second), form3])
        mask, sums = 1, [total]
        while mask < n_gy:
            total = total + swap(total, "gy", mask)
            sums.append(total)
            mask *= 2
        total += sum(swap(total, "gx", m) for m in range(1, n_gx))
        forms.append(total)
        return sums[0], sums[-1]

    third = apply_operator(second, first, 2.0, add_forms)
    return (forms[0], jnp.concatenate(third))


def solution(mesh):
    return jax.shard_map(
        body,
        mesh=mesh,
        in_specs=(
            P("gy", "gx", None, None, None),
            P("gy", "gx", None),
            P("gy", "gx", None),
            P(("gy", "gx"), "gz"),
            P(("gy", "gx")),
        ),
        out_specs=(P(None, "gz"), P(("gy", "gx"), "gz")),
        check_vma=False,
    )
```

```python
import functools

import jax
import jax.numpy as jnp
from jax import lax
from jax.experimental import pallas as pl
from jax.experimental.pallas import tpu as pltpu
from jax.sharding import PartitionSpec as P


WIDE, NARROW = 16, 8
PARTS, DEPTH = 16, 6
VMEM = pl.BlockSpec(memory_space=pltpu.VMEM)
ANY = pl.BlockSpec(memory_space=pl.ANY)
HBM = pl.BlockSpec(memory_space=pltpu.HBM)
PARAMS = pltpu.CompilerParams(vmem_limit_bytes=24 << 20)


def swap(value, axis, mask):
    n = lax.axis_size(axis)
    return lax.ppermute(value, axis, [(d, d ^ mask) for d in range(n)])


def after(value, gate):
    return lax.optimization_barrier((value, gate))[0]


class Layout:
    def __init__(self, kt, size, probes, rb, n_gx, n_gy):
        self.kt, self.size, self.probes, self.rb, self.n_gx, self.n_gy = kt, size, probes, rb, n_gx, n_gy
        self.top, self.dests = n_gy // 2, n_gx // 2
        small = max(rb // 4, 1)
        self.chunks = [rb - rb // 2, rb // 2]
        self.starts = [sum(self.chunks[:c]) for c in range(len(self.chunks))]
        self.steps = (WIDE, WIDE, NARROW, NARROW)
        tail = self.chunks[-1]
        self.last = rb - tail
        self.fields = (self.top * self.last, self.top * rb, self.top * tail, self.top * tail)
        self.firsts = (0, 0, self.dests * rb, 0)
        self.slots = -(-(kt + sum(self.steps)) // 128) * 128

    def place(self, block_rows, block_cols):
        rb, here_x, here_y = self.rb, lax.axis_index("gx"), lax.axis_index("gy")
        dest, q = (block_rows // rb) ^ here_x, block_rows % rb
        piece, blk = (block_cols // rb) ^ here_y, block_cols % rb
        send = dest % 2
        row = send * (self.dests * rb)
        col = jnp.zeros_like(blk)
        for start, count in zip(self.starts, self.chunks):
            inside = (q >= start) & (q < start + count)
            row += jnp.where(inside, self.dests * start + dest // 2 * count + q - start, 0)
            inside = (blk >= start) & (blk < start + count)
            col += jnp.where(inside, self.top * start + piece % self.top * count + blk - start, 0)
        near, soon = piece < self.top, blk < self.last
        col -= jnp.where(near | soon, 0, self.top * self.last)
        which = jnp.where(near & soon, 0, jnp.where(near | soon, 1, 3 - send))
        return which, col, row


def start_kernel(lay, tables_hbm, blocks_hbm, *refs):
    pieces, (blocks_ref, plan_ref, total, tables_ref, field, planned, sem) = refs[:-7], refs[-7:]
    kt, parts = lay.kt, sem.shape[0] - 2
    part = kt // parts

    def copy(p):
        cut = pl.ds(p * part, part)
        return pltpu.make_async_copy(blocks_hbm.at[cut], blocks_ref.at[cut], sem.at[p])

    tables = pltpu.make_async_copy(tables_hbm, tables_ref, sem.at[parts])
    tables.start()
    for p in range(DEPTH):
        copy(p).start()
    total[...] = jnp.zeros_like(total)
    tables.wait()
    down, along = (lax.broadcasted_iota(jnp.int32, (kt, kt), d) for d in (0, 1))
    upright = lambda v: jnp.sum(jnp.where(down == along, v, 0), axis=1, keepdims=True)
    flat = lay.place(tables_ref[0:1, :], tables_ref[1:2, :])
    which, col, row = (upright(v) for v in flat)
    rank = jnp.sum(((flat[0] == which) & (along < down)).astype(jnp.int32), axis=1, keepdims=True)
    slots = lax.broadcasted_iota(jnp.int32, (1, lay.slots), 1)
    place, base = rank, jnp.zeros((1, 1), jnp.int32)
    fill_col, fill_row = jnp.zeros_like(slots), jnp.zeros_like(slots)
    sizes = jnp.zeros_like(slots)
    for number, step in enumerate(lay.steps):
        count = jnp.sum((flat[0] == number).astype(jnp.int32), axis=1, keepdims=True)
        trips = (count + step - 1) // step
        place += jnp.where(which == number, base, 0)
        end = base + trips * step
        inside = (slots >= base) & (slots < end)
        fill_col += jnp.where(inside, lay.fields[number], 0)
        fill_row += jnp.where(inside, lay.firsts[number], 0)
        sizes += jnp.where(slots == 2 * number, base, 0) + jnp.where(slots == 2 * number + 1, trips, 0)
        base = end
    hit = place == slots
    pick = lambda v: jnp.sum(jnp.where(hit, v, 0), axis=0, keepdims=True)
    empty = 1 - pick(1)
    plan_ref[0:1, :] = pick(lax.broadcasted_iota(jnp.int32, (kt, 1), 0))
    plan_ref[1:2, :] = pick(col) + empty * fill_col
    plan_ref[2:3, :] = pick(row) + empty * fill_row
    plan_ref[3:4, :] = sizes

    def arrive(p, carry):
        copy(p).wait()

        @pl.when(p + DEPTH < parts)
        def _():
            copy(p + DEPTH).start()

        return carry

    def await_step(at, step, arrived):
        need = planned[0, at]
        for u in range(1, step):
            need = jnp.maximum(need, planned[0, at + u])
        need = jnp.maximum(need // part + 1, arrived)
        lax.fori_loop(arrived, need, arrive, 0)
        return need

    def prepare():
        pass

    arrived = run_list(lay, 0, plan_ref, blocks_ref, pieces, field, total, planned, sem.at[parts + 1], prepare, await_step)
    lax.fori_loop(arrived, parts, arrive, 0)


def run_list(lay, number, plan_hbm, blocks_ref, pieces, field, total, plan_ref, sem, prepare, await_step=None):
    size, first_row, step = lay.size, lay.firsts[number], lay.steps[number]
    fetch = pltpu.make_async_copy(plan_hbm, plan_ref, sem)
    fetch.start()
    prepare()
    place = 0
    for piece in pieces:
        field[pl.ds(place, piece.shape[0]), :] = piece[...]
        place += piece.shape[0]
    field[pl.ds(place, size), :] = jnp.zeros((size, lay.probes), field.dtype)
    fetch.wait()
    start = plan_ref[3, 2 * number]

    def go(it, carry):
        if await_step:
            carry = await_step(start + it * step, step, carry)
        for u in range(step):
            at = start + it * step + u
            part = jnp.dot(
                blocks_ref[plan_ref[0, at]],
                field[pl.ds(pl.multiple_of(plan_ref[1, at] * size, size), size), :],
                preferred_element_type=jnp.float32,
            )
            total[plan_ref[2, at] - first_row] += part
        return carry

    return lax.fori_loop(0, plan_ref[3, 2 * number + 1], go, 0)


def early_kernel(lay, number, plan_hbm, blocks_ref, *refs):
    before, refs = (refs[0], refs[1:]) if number else (None, refs)
    *pieces, total, field, plan_ref, sem = refs

    def prepare():
        total[...] = jnp.zeros_like(total) if before is None else before[...]

    run_list(lay, number, plan_hbm, blocks_ref, pieces, field, total, plan_ref, sem, prepare)


def late_kernel(lay, number, plan_hbm, blocks_ref, before, *refs):
    pieces, outs = refs[: lay.top], refs[lay.top : -4]
    field, total, plan_ref, sem = refs[-4:]

    def prepare():
        total[...] = before[pl.ds(lay.firsts[number], total.shape[0])]

    run_list(lay, number, plan_hbm, blocks_ref, pieces, field, total, plan_ref, sem, prepare)
    for out, start, count in zip(outs, lay.starts, lay.chunks):
        part = total[pl.ds(lay.dests * start, lay.dests * count)]
        out[...] = part.reshape(out.shape).astype(out.dtype)


def body(blocks, block_rows, block_cols, probe_bits, shift):
    kt, size, _ = blocks.shape[2:]
    local_rows, probes = probe_bits.shape
    n_gx, n_gy = lax.axis_size("gx"), lax.axis_size("gy")
    lay = Layout(kt, size, probes, local_rows // size, n_gx, n_gy)
    chunks = range(len(lay.chunks))

    def cost(share):
        return pl.CostEstimate(
            flops=int(2 * kt * size * size * probes * share), bytes_accessed=0, transcendentals=0
        )

    cut = lambda v: [v[s * size : (s + n) * size] for s, n in zip(lay.starts, lay.chunks)]
    signs = [(2 * v - 1).astype(jnp.float32) for v in cut(probe_bits)]
    scale = [v[:, None] for v in cut(shift)]

    begin = pl.pallas_call(
        functools.partial(start_kernel, lay),
        out_shape=(
            jax.ShapeDtypeStruct((kt, size, size), blocks.dtype),
            jax.ShapeDtypeStruct((4, lay.slots), jnp.int32),
            jax.ShapeDtypeStruct((n_gx * lay.rb, size, probes), jnp.float32),
        ),
        in_specs=[ANY, ANY] + [VMEM] * (lay.top * (len(lay.chunks) - 1)),
        out_specs=(VMEM, VMEM, VMEM),
        scratch_shapes=[
            pltpu.VMEM((2, kt), jnp.int32),
            pltpu.VMEM(((lay.fields[0] + 1) * size, probes), jnp.bfloat16),
            pltpu.SMEM((4, lay.slots), jnp.int32),
            pltpu.SemaphoreType.DMA((PARTS + 2,)),
        ],
        compiler_params=PARAMS,
        cost_estimate=cost(1.0),
        name="start",
    )
    tables = jnp.concatenate([block_rows[0], block_cols[0]])
    stored = []

    def spread(pieces):
        own, mask = {0: pieces}, lay.top // 2
        while mask:
            own.update({m | mask: swap(v, "gy", mask) for m, v in own.items()})
            mask //= 2
        return [own[m] for m in range(lay.top)]

    fetched = [pltpu.SMEM((4, lay.slots), jnp.int32), pltpu.SemaphoreType.DMA]

    def early(number, before, pieces, share):
        return pl.pallas_call(
            functools.partial(early_kernel, lay, number),
            out_shape=jax.ShapeDtypeStruct((n_gx * lay.rb, size, probes), jnp.float32),
            in_specs=[ANY, VMEM] + [VMEM] * (len(before) + len(pieces)),
            out_specs=VMEM,
            scratch_shapes=[pltpu.VMEM(((lay.fields[number] + 1) * size, probes), jnp.bfloat16)] + fetched,
            compiler_params=PARAMS,
            cost_estimate=cost(share),
        )(*stored, *before, *pieces)

    def late(number, dtype, before, pieces, share):
        return pl.pallas_call(
            functools.partial(late_kernel, lay, number),
            out_shape=tuple(jax.ShapeDtypeStruct((lay.dests * n * size, probes), dtype) for n in lay.chunks),
            in_specs=[ANY, VMEM, VMEM] + [VMEM] * len(pieces),
            out_specs=(VMEM,) * len(lay.chunks),
            scratch_shapes=[
                pltpu.VMEM(((lay.fields[number] + 1) * size, probes), jnp.bfloat16),
                pltpu.VMEM((lay.dests * lay.rb, size, probes), jnp.float32),
            ]
            + fetched,
            compiler_params=PARAMS,
            cost_estimate=cost(share),
        )(*stored, before, *pieces)

    def multiply(it, field):
        across = [swap(v, "gy", lay.top) for v in field]
        near = [spread(v) for v in field]
        far = [spread(v) for v in across[:-1]]
        if stored:
            total = early(0, [], sum(near[:-1], []), 0.25)
        else:
            held, plan, total = begin(tables, blocks[0, 0], *sum(near[:-1], []))
            stored.extend((plan, held))
        total = early(1, [total], sum(far, []) + near[-1], 0.5)
        rest = spread(after(across[-1], total) if it else across[-1])
        send = late(2, jnp.bfloat16, total, rest, 0.12)
        return send, late(3, jnp.float32, total, rest, 0.12)

    def reduce(send, keep, gate=None):
        send, keep, last = list(send), list(keep), [None] * len(send)
        mask, width = 1, n_gx // 2
        while True:
            got = [swap(v, "gx", mask) for v in send]
            mask *= 2
            if mask == n_gx and gate is not None:
                sums = gate(last)
                got[0] = after(got[0], sums[0])
                got[-1] = after(got[-1], sums[1])
            for c in chunks:
                if c:
                    got[c] = after(got[c], send[c - 1] if mask < n_gx else keep[c - 1])
                keep[c] = keep[c] + got[c].astype(jnp.float32)
                if mask < n_gx:
                    parts = keep[c].reshape(width // 2, 2, -1, probes)
                    keep[c] = parts[:, 0].reshape(-1, probes)
                    gone = parts[:, 1].reshape(-1, probes)
                    last[c] = (keep[c], gone)
                    send[c] = gone.astype(jnp.bfloat16)
            width //= 2
            if mask == n_gx:
                return keep

    def apply_operator(it, field, previous, factor, gate=None):
        send, keep = multiply(it, [v.astype(jnp.bfloat16) for v in field])
        sums = reduce(send, keep, gate)
        out = []
        for s, d, v, u in zip(sums, scale, field, previous):
            if out:
                s = after(s, out[-1].astype(jnp.bfloat16))
            term = factor * (s + d * v)
            out.append(term if u is None else term - u)
        return out

    def dot(us, vs):
        return sum(jnp.sum(u * v, axis=0) for u, v in zip(us, vs))

    far_signs = jnp.concatenate([v.astype(jnp.bfloat16) for v in signs])
    far_signs = swap(far_signs, "gx", n_gx // 2)
    far_signs = [v.astype(jnp.float32) for v in cut(far_signs)]
    first = apply_operator(0, signs, [None] * len(signs), 1.0)
    second = apply_operator(1, first, signs, 2.0)
    forms = []

    def add_forms(last):
        rest = [2.0 * d * v - u for d, v, u in zip(scale, second, first)]
        form3 = dot(signs, rest)
        form3 += 2.0 * (dot(signs, [v[0] for v in last]) + dot(far_signs, [v[1] for v in last]))
        total = jnp.stack([dot(signs, first), dot(signs, second), form3])
        mask, sums = 1, [total]
        while mask < n_gy:
            total = total + swap(total, "gy", mask)
            sums.append(total)
            mask *= 2
        mask = 1
        while mask < n_gx:
            total = total + swap(total, "gx", mask)
            mask *= 2
        forms.append(total)
        return sums[0], sums[-1]

    third = apply_operator(2, second, first, 2.0, add_forms)
    return (forms[0], jnp.concatenate(third))


def solution(mesh):
    return jax.shard_map(
        body,
        mesh=mesh,
        in_specs=(
            P("gy", "gx", None, None, None),
            P("gy", "gx", None),
            P("gy", "gx", None),
            P(("gy", "gx"), "gz"),
            P(("gy", "gx")),
        ),
        out_specs=(P(None, "gz"), P(("gy", "gx"), "gz")),
        check_vma=False,
    )
```

```python
import functools

import jax
import jax.numpy as jnp
from jax import lax
from jax.experimental import pallas as pl
from jax.experimental.pallas import tpu as pltpu
from jax.sharding import PartitionSpec as P


WIDE, NARROW = 16, 8
PARTS, DEPTH = 16, 6
VMEM = pl.BlockSpec(memory_space=pltpu.VMEM)
ANY = pl.BlockSpec(memory_space=pl.ANY)
HBM = pl.BlockSpec(memory_space=pltpu.HBM)
PARAMS = pltpu.CompilerParams(vmem_limit_bytes=24 << 20)


def swap(value, axis, mask):
    n = lax.axis_size(axis)
    return lax.ppermute(value, axis, [(d, d ^ mask) for d in range(n)])


def after(value, gate):
    return lax.optimization_barrier((value, gate))[0]


class Layout:
    def __init__(self, kt, size, probes, rb, n_gx, n_gy):
        self.kt, self.size, self.probes, self.rb, self.n_gx, self.n_gy = kt, size, probes, rb, n_gx, n_gy
        self.top, self.dests = n_gy // 2, n_gx // 2
        small = max(rb // 4, 1)
        self.chunks = [rb - rb // 2, rb // 2]
        self.starts = [sum(self.chunks[:c]) for c in range(len(self.chunks))]
        self.steps = (WIDE, WIDE, NARROW, NARROW)
        tail = self.chunks[-1]
        self.last = rb - tail
        self.fields = (self.top * self.last, self.top * rb, self.top * tail, self.top * tail)
        self.firsts = (0, 0, self.dests * rb, 0)
        self.slots = -(-(kt + sum(self.steps)) // 128) * 128

    def place(self, block_rows, block_cols):
        rb, here_x, here_y = self.rb, lax.axis_index("gx"), lax.axis_index("gy")
        dest, q = (block_rows // rb) ^ here_x, block_rows % rb
        piece, blk = (block_cols // rb) ^ here_y, block_cols % rb
        send = dest % 2
        row = send * (self.dests * rb)
        col = jnp.zeros_like(blk)
        for start, count in zip(self.starts, self.chunks):
            inside = (q >= start) & (q < start + count)
            row += jnp.where(inside, self.dests * start + dest // 2 * count + q - start, 0)
            inside = (blk >= start) & (blk < start + count)
            col += jnp.where(inside, self.top * start + piece % self.top * count + blk - start, 0)
        near, soon = piece < self.top, blk < self.last
        col -= jnp.where(near | soon, 0, self.top * self.last)
        which = jnp.where(near & soon, 0, jnp.where(near | soon, 1, 3 - send))
        return which, col, row


def start_kernel(lay, tables_hbm, blocks_hbm, *refs):
    pieces, (blocks_ref, plan_ref, total, tables_ref, field, planned, sem) = refs[:-7], refs[-7:]
    kt, parts = lay.kt, sem.shape[0] - 2
    part = kt // parts

    def copy(p):
        cut = pl.ds(p * part, part)
        return pltpu.make_async_copy(blocks_hbm.at[cut], blocks_ref.at[cut], sem.at[p])

    tables = pltpu.make_async_copy(tables_hbm, tables_ref, sem.at[parts])
    tables.start()
    for p in range(DEPTH):
        copy(p).start()
    total[...] = jnp.zeros_like(total)
    tables.wait()
    down, along = (lax.broadcasted_iota(jnp.int32, (kt, kt), d) for d in (0, 1))
    upright = lambda v: jnp.sum(jnp.where(down == along, v, 0), axis=1, keepdims=True)
    flat = lay.place(tables_ref[0:1, :], tables_ref[1:2, :])
    which, col, row = (upright(v) for v in flat)
    rank = jnp.sum(((flat[0] == which) & (along < down)).astype(jnp.int32), axis=1, keepdims=True)
    slots = lax.broadcasted_iota(jnp.int32, (1, lay.slots), 1)
    place, base = rank, jnp.zeros((1, 1), jnp.int32)
    fill_col, fill_row = jnp.zeros_like(slots), jnp.zeros_like(slots)
    sizes = jnp.zeros_like(slots)
    for number, step in enumerate(lay.steps):
        count = jnp.sum((flat[0] == number).astype(jnp.int32), axis=1, keepdims=True)
        trips = (count + step - 1) // step
        place += jnp.where(which == number, base, 0)
        end = base + trips * step
        inside = (slots >= base) & (slots < end)
        fill_col += jnp.where(inside, lay.fields[number], 0)
        fill_row += jnp.where(inside, lay.firsts[number], 0)
        sizes += jnp.where(slots == 2 * number, base, 0) + jnp.where(slots == 2 * number + 1, trips, 0)
        base = end
    hit = place == slots
    pick = lambda v: jnp.sum(jnp.where(hit, v, 0), axis=0, keepdims=True)
    empty = 1 - pick(1)
    plan_ref[0:1, :] = pick(lax.broadcasted_iota(jnp.int32, (kt, 1), 0))
    plan_ref[1:2, :] = pick(col) + empty * fill_col
    plan_ref[2:3, :] = pick(row) + empty * fill_row
    plan_ref[3:4, :] = sizes

    def arrive(p, carry):
        copy(p).wait()

        @pl.when(p + DEPTH < parts)
        def _():
            copy(p + DEPTH).start()

        return carry

    def await_step(at, step, arrived):
        need = planned[0, at]
        for u in range(1, step):
            need = jnp.maximum(need, planned[0, at + u])
        need = jnp.maximum(need // part + 1, arrived)
        lax.fori_loop(arrived, need, arrive, 0)
        return need

    def prepare():
        pass

    arrived = run_list(lay, 0, plan_ref, blocks_ref, pieces, field, total, planned, sem.at[parts + 1], prepare, await_step)
    lax.fori_loop(arrived, parts, arrive, 0)


def run_list(lay, number, plan_hbm, blocks_ref, pieces, field, total, plan_ref, sem, prepare, await_step=None):
    size, first_row, step = lay.size, lay.firsts[number], lay.steps[number]
    fetch = pltpu.make_async_copy(plan_hbm, plan_ref, sem)
    fetch.start()
    prepare()
    place = 0
    for piece in pieces:
        field[pl.ds(place, piece.shape[0]), :] = piece[...]
        place += piece.shape[0]
    field[pl.ds(place, size), :] = jnp.zeros((size, lay.probes), field.dtype)
    fetch.wait()
    start = plan_ref[3, 2 * number]

    def go(it, carry):
        if await_step:
            carry = await_step(start + it * step, step, carry)
        for u in range(step):
            at = start + it * step + u
            part = jnp.dot(
                blocks_ref[plan_ref[0, at]],
                field[pl.ds(pl.multiple_of(plan_ref[1, at] * size, size), size), :],
                preferred_element_type=jnp.float32,
            )
            total[plan_ref[2, at] - first_row] += part
        return carry

    return lax.fori_loop(0, plan_ref[3, 2 * number + 1], go, 0)


def early_kernel(lay, number, plan_hbm, blocks_ref, *refs):
    before, refs = (refs[0], refs[1:]) if number else (None, refs)
    *pieces, total, field, plan_ref, sem = refs

    def prepare():
        total[...] = jnp.zeros_like(total) if before is None else before[...]

    run_list(lay, number, plan_hbm, blocks_ref, pieces, field, total, plan_ref, sem, prepare)


def late_kernel(lay, number, plan_hbm, blocks_ref, before, *refs):
    pieces, outs = refs[: lay.top], refs[lay.top : -4]
    field, total, plan_ref, sem = refs[-4:]

    def prepare():
        total[...] = before[pl.ds(lay.firsts[number], total.shape[0])]

    run_list(lay, number, plan_hbm, blocks_ref, pieces, field, total, plan_ref, sem, prepare)
    for out, start, count in zip(outs, lay.starts, lay.chunks):
        part = total[pl.ds(lay.dests * start, lay.dests * count)]
        out[...] = part.reshape(out.shape).astype(out.dtype)


def body(blocks, block_rows, block_cols, probe_bits, shift):
    kt, size, _ = blocks.shape[2:]
    local_rows, probes = probe_bits.shape
    n_gx, n_gy = lax.axis_size("gx"), lax.axis_size("gy")
    lay = Layout(kt, size, probes, local_rows // size, n_gx, n_gy)
    chunks = range(len(lay.chunks))

    def cost(share):
        return pl.CostEstimate(
            flops=int(2 * kt * size * size * probes * share), bytes_accessed=0, transcendentals=0
        )

    cut = lambda v: [v[s * size : (s + n) * size] for s, n in zip(lay.starts, lay.chunks)]
    signs = [(2 * v - 1).astype(jnp.float32) for v in cut(probe_bits)]
    scale = [v[:, None] for v in cut(shift)]

    begin = pl.pallas_call(
        functools.partial(start_kernel, lay),
        out_shape=(
            jax.ShapeDtypeStruct((kt, size, size), blocks.dtype),
            jax.ShapeDtypeStruct((4, lay.slots), jnp.int32),
            jax.ShapeDtypeStruct((n_gx * lay.rb, size, probes), jnp.float32),
        ),
        in_specs=[ANY, ANY] + [VMEM] * (lay.top * (len(lay.chunks) - 1)),
        out_specs=(VMEM, VMEM, VMEM),
        scratch_shapes=[
            pltpu.VMEM((2, kt), jnp.int32),
            pltpu.VMEM(((lay.fields[0] + 1) * size, probes), jnp.bfloat16),
            pltpu.SMEM((4, lay.slots), jnp.int32),
            pltpu.SemaphoreType.DMA((PARTS + 2,)),
        ],
        compiler_params=PARAMS,
        cost_estimate=cost(1.0),
        name="start",
    )
    tables = jnp.concatenate([block_rows[0], block_cols[0]])
    stored = []

    def spread(pieces):
        own, mask = {0: pieces}, lay.top // 2
        while mask:
            own.update({m | mask: swap(v, "gy", mask) for m, v in own.items()})
            mask //= 2
        return [own[m] for m in range(lay.top)]

    fetched = [pltpu.SMEM((4, lay.slots), jnp.int32), pltpu.SemaphoreType.DMA]

    def early(number, before, pieces, share):
        return pl.pallas_call(
            functools.partial(early_kernel, lay, number),
            out_shape=jax.ShapeDtypeStruct((n_gx * lay.rb, size, probes), jnp.float32),
            in_specs=[ANY, VMEM] + [VMEM] * (len(before) + len(pieces)),
            out_specs=VMEM,
            scratch_shapes=[pltpu.VMEM(((lay.fields[number] + 1) * size, probes), jnp.bfloat16)] + fetched,
            compiler_params=PARAMS,
            cost_estimate=cost(share),
        )(*stored, *before, *pieces)

    def late(number, dtype, before, pieces, share):
        return pl.pallas_call(
            functools.partial(late_kernel, lay, number),
            out_shape=tuple(jax.ShapeDtypeStruct((lay.dests * n * size, probes), dtype) for n in lay.chunks),
            in_specs=[ANY, VMEM, VMEM] + [VMEM] * len(pieces),
            out_specs=(VMEM,) * len(lay.chunks),
            scratch_shapes=[
                pltpu.VMEM(((lay.fields[number] + 1) * size, probes), jnp.bfloat16),
                pltpu.VMEM((lay.dests * lay.rb, size, probes), jnp.float32),
            ]
            + fetched,
            compiler_params=PARAMS,
            cost_estimate=cost(share),
        )(*stored, before, *pieces)

    def multiply(it, field):
        across = [swap(v, "gy", lay.top) for v in field]
        near = [spread(v) for v in field]
        far = [spread(v) for v in across[:-1]]
        if stored:
            total = early(0, [], sum(near[:-1], []), 0.25)
        else:
            held, plan, total = begin(tables, blocks[0, 0], *sum(near[:-1], []))
            stored.extend((plan, held))
        total = early(1, [total], sum(far, []) + near[-1], 0.5)
        rest = spread(after(across[-1], total) if it else across[-1])
        send = late(2, jnp.bfloat16, total, rest, 0.12)
        return send, late(3, jnp.float32, total, rest, 0.12)

    def reduce(send, keep, gate=None):
        send, keep, last = list(send), list(keep), [None] * len(send)
        mask, width = 1, n_gx // 2
        while True:
            got = [swap(v, "gx", mask) for v in send]
            mask *= 2
            if mask == n_gx and gate is not None:
                sums = gate(last)
                got[0] = after(got[0], sums[0])
                got[-1] = after(got[-1], sums[1])
            for c in chunks:
                if c:
                    got[c] = after(got[c], send[c - 1] if mask < n_gx else keep[c - 1])
                keep[c] = keep[c] + got[c].astype(jnp.float32)
                if mask < n_gx:
                    parts = keep[c].reshape(width // 2, 2, -1, probes)
                    keep[c] = parts[:, 0].reshape(-1, probes)
                    gone = parts[:, 1].reshape(-1, probes)
                    last[c] = (keep[c], gone)
                    send[c] = gone.astype(jnp.bfloat16)
            width //= 2
            if mask == n_gx:
                return keep

    def apply_operator(it, field, previous, factor, gate=None):
        send, keep = multiply(it, [v.astype(jnp.bfloat16) for v in field])
        sums = reduce(send, keep, gate)
        out = []
        for s, d, v, u in zip(sums, scale, field, previous):
            if out:
                s = after(s, out[-1].astype(jnp.bfloat16))
            term = factor * (s + d * v)
            out.append(term if u is None else term - u)
        return out

    def dot(us, vs):
        return sum(jnp.sum(u * v, axis=0) for u, v in zip(us, vs))

    far_signs = jnp.concatenate([v.astype(jnp.bfloat16) for v in signs])
    far_signs = swap(far_signs, "gx", n_gx // 2)
    far_signs = [v.astype(jnp.float32) for v in cut(far_signs)]
    first = apply_operator(0, signs, [None] * len(signs), 1.0)
    second = apply_operator(1, first, signs, 2.0)
    forms = []

    def add_forms(last):
        rest = [2.0 * d * v - u for d, v, u in zip(scale, second, first)]
        form3 = dot(signs, rest)
        form3 += 2.0 * (dot(signs, [v[0] for v in last]) + dot(far_signs, [v[1] for v in last]))
        total = jnp.stack([dot(signs, first), dot(signs, second), form3])
        mask, sums = 1, [total]
        while mask < lay.top:
            total = total + swap(total, "gy", mask)
            mask *= 2
        total = total + swap(total, "gy", lay.top) + swap(total, "gx", 1) + swap(total, ("gx", "gy"), n_gy + lay.top)
        sums.append(total)
        mask = 2
        while mask < n_gx:
            got = swap(total, "gx", mask)
            mask *= 2
            if mask < n_gx:
                total = total + got
        forms.extend((total, got))
        return sums[0], sums[-1]

    third = apply_operator(2, second, first, 2.0, add_forms)
    third = jnp.concatenate(third)
    return (forms[0] + after(forms[1], third), third)


def solution(mesh):
    return jax.shard_map(
        body,
        mesh=mesh,
        in_specs=(
            P("gy", "gx", None, None, None),
            P("gy", "gx", None),
            P("gy", "gx", None),
            P(("gy", "gx"), "gz"),
            P(("gy", "gx")),
        ),
        out_specs=(P(None, "gz"), P(("gy", "gx"), "gz")),
        check_vma=False,
    )
```
